128 devices in a mesh: dp: 16 (over y, x), mp: 8 (over z, core).
Axes of the slice: x: 4, y: 4, z: 4, core: 2. Of those that a mesh axis runs over, the one named last changes fastest.
Arguments:
- stored: float32 [16384, 18432], P(('dp', 'mp')), may hold values from -0.046875 to 0.046875
- row_map: int32 [16384], replicated, may hold values from 0 to 16383, as said below
- probe: bfloat16 [16384, 1024], P('dp'), may hold values from -6 to 6
- lane: bfloat16 [128, 1024], replicated, may hold values from -6 to 6
Outputs:
- shards: bfloat16 [144, 128, 16384], P('mp', None, 'dp')
- slab_checks: float32 [144, 128, 1024], P('mp', 'dp')
- head_sums: float32 [144, 1024], P('mp')
The draws below stay inside these ranges and needn't reach their ends.
Inputs may be any that keep to these rules, and one draw needn't show every extreme that they name: row_map is a permutation of 0..16383 with row_map[i] // 1024 == (i % 128) // 8 for every stored row i.
All inputs are finite; a program needn't handle non-finite values.
Results may differ from the reference program's by a relative error of at most 0.0029.
Values may be sent and summed in bfloat16 or wider, within the bound.
No kernel may reach another device: no remote copies, remote signals or barrier semaphores. Data moves between devices by JAX's collectives and lax.ppermute only.
A program may use at most 64 MiB of HBM per device.

```python
import jax
import jax.numpy as jnp
from jax import lax

D = 16384
Q_HEADS = 128
KV_HEADS = 8
HD = 128
PROBES = 1024
SLABS = 8
QKV = 18432
ROWS_DEV = 128
SUB_ROWS = 8
GROUP_ROWS = 1024
DP_GROUPS = 16
SLAB = 128
SLOTS = 18
N_DP = 16
N_MP = 8


def draw_row_map(key, part):
    stored_index = jnp.arange(D, dtype=jnp.int32)
    target_group = stored_index % ROWS_DEV // SUB_ROWS
    rank_inside = stored_index // ROWS_DEV * SUB_ROWS + stored_index % SUB_ROWS
    group_keys = jax.random.split(jax.random.fold_in(key, 17), DP_GROUPS)
    shuffled = jax.vmap(lambda one_key: jax.random.permutation(one_key, GROUP_ROWS))(group_keys).astype(jnp.int32)
    return (target_group * GROUP_ROWS + shuffled[target_group, rank_inside]).astype(jnp.int32)


def levels(rng, dims, pieces, least, high):
    def one(axis_at, blocks):
        heights = jax.random.uniform(jax.random.fold_in(jax.random.fold_in(rng, 6), axis_at), (blocks,), jnp.float32, least / len(pieces), high / len(pieces))
        return jnp.repeat(jnp.exp(heights), dims[axis_at] // blocks).reshape((-1,) + (1,) * (len(dims) - axis_at - 1))

    factor_of = one(*pieces[0])
    for cut in pieces[1:]:
        factor_of = factor_of * one(*cut)
    return factor_of


def scatter_about(stream_key, dims, deviation, reach, cuts=(), kind=jnp.bfloat16):
    entries = deviation * jax.random.normal(stream_key, dims, jnp.float32)
    if cuts:
        entries = entries * levels(stream_key, dims, cuts, -0.22, 0.18)
    return jnp.clip(entries, -reach, reach).astype(kind)


def setup_inputs(seed: int = 0) -> dict:
    arg_keys = jax.random.split(jax.random.key(seed), 5)
    return {
        "stored": scatter_about(arg_keys[0], (D, QKV), D ** -0.5, 0.046875, ((0, 128),), jnp.float32),
        "row_map": draw_row_map(jax.random.fold_in(arg_keys[4], 71), 0),
        "probe": scatter_about(arg_keys[2], (D, PROBES), 1.0, 6.0, ((0, 16),)),
        "lane": scatter_about(arg_keys[3], (HD, PROBES), 1.0, 6.0),
    }


def reference(stored, row_map, probe, lane):
    weights = jnp.zeros((D, QKV), jnp.bfloat16).at[row_map].set(stored.astype(jnp.bfloat16))
    head_cols = weights.reshape(D, Q_HEADS + 2 * KV_HEADS, HD)
    kv_index = (jnp.arange(N_MP, dtype=jnp.int32) * KV_HEADS) // N_MP
    query_cols = head_cols[:, :Q_HEADS].reshape(D, N_MP, Q_HEADS // N_MP, HD)
    key_cols = head_cols[:, Q_HEADS + kv_index][:, :, None]
    value_cols = head_cols[:, Q_HEADS + KV_HEADS + kv_index][:, :, None]
    slotted = jnp.concatenate([query_cols, key_cols, value_cols], axis=2)
    shards = jnp.transpose(slotted, (1, 2, 3, 0)).reshape(N_MP * SLOTS, HD, D)
    lane_wide = lane.astype(jnp.float32)

    def one_slab(slab_start):
        slab_block = lax.dynamic_slice_in_dim(shards, slab_start, SLAB, 2).astype(jnp.float32)
        probe_rows = lax.dynamic_slice_in_dim(probe, slab_start, SLAB, 0).astype(jnp.float32)
        projected = jnp.einsum("jer,rp->jep", slab_block, probe_rows, precision=lax.Precision.HIGHEST)
        return jnp.sum(projected * lane_wide[None], axis=1)

    slab_starts = jnp.arange(N_DP * SLABS, dtype=jnp.int32) * SLAB
    stacked = lax.map(one_slab, slab_starts)
    slab_checks = jnp.transpose(stacked, (1, 0, 2))
    head_sums = jnp.mean(slab_checks, axis=1)
    return shards, slab_checks, head_sums
```

```python
import jax
import jax.numpy as jnp
from jax import lax
from jax.experimental import pallas as pl
from jax.experimental.pallas import tpu as pltpu
from jax.sharding import Mesh
from jax.sharding import PartitionSpec as P

Q_HEADS = 128
KV_HEADS = 8
HD = 128
PROBES = 1024
SLABS = 8
N_DP = 16
N_MP = 8
PER_DEVICE = Q_HEADS // N_MP
SLOTS = PER_DEVICE + 2
SUB_ROWS = 8
ROWS_DEV = 128
GROUP_ROWS = 1024
SLAB_ROWS = GROUP_ROWS // SLABS
DP = ("dp_0", "dp_1")
DP_MP = ("dp_0", "dp_1", "mp")
STEP_HEADS = 3


def pack_kernel(query_ref, key_ref, value_ref, out_ref):
    wide = PER_DEVICE * HD
    query = query_ref[...].reshape(N_DP, SUB_ROWS, wide)
    key = key_ref[...].reshape(N_DP, SUB_ROWS, HD)
    value = value_ref[...].reshape(N_DP, SUB_ROWS, HD)
    out_ref[:, 0, :, :wide] = query.astype(jnp.bfloat16)
    out_ref[:, 0, :, wide : wide + HD] = key.astype(jnp.bfloat16)
    out_ref[:, 0, :, wide + HD :] = value.astype(jnp.bfloat16)


def pack(stored):
    return pl.pallas_call(
        pack_kernel,
        grid=(N_MP,),
        in_specs=[
            pl.BlockSpec((ROWS_DEV, PER_DEVICE * HD), lambda m: (0, m)),
            pl.BlockSpec((ROWS_DEV, HD), lambda m: (0, Q_HEADS + m)),
            pl.BlockSpec((ROWS_DEV, HD), lambda m: (0, Q_HEADS + KV_HEADS + m)),
        ],
        out_specs=pl.BlockSpec(
            (N_DP, 1, SUB_ROWS, SLOTS * HD), lambda m: (0, m, 0, 0)
        ),
        out_shape=jax.ShapeDtypeStruct(
            (N_DP, N_MP, SUB_ROWS, SLOTS * HD), jnp.bfloat16
        ),
        name="pack",
    )(stored, stored, stored)


def finish_kernel(arrived_ref, place_ref, probe_ref, lane_ref, shards_ref, checks_ref):
    placed = lax.dot_general(
        arrived_ref[...],
        place_ref[...],
        (((0,), (0,)), ((), ())),
        preferred_element_type=jnp.float32,
    ).astype(jnp.bfloat16)
    shards_ref[...] = placed.reshape(STEP_HEADS, HD, GROUP_ROWS)
    lane_wide = lane_ref[...].astype(jnp.float32)
    for slab in range(SLABS):
        rows = slice(slab * SLAB_ROWS, (slab + 1) * SLAB_ROWS)
        projected = jnp.dot(
            placed[:, rows], probe_ref[rows, :], preferred_element_type=jnp.float32
        ).reshape(STEP_HEADS, HD, PROBES)
        checks_ref[:, slab, :] = jnp.sum(projected * lane_wide[None], axis=1)


def finish(arrived, place, probe, lane):
    vmem = pl.BlockSpec(memory_space=pltpu.VMEM)
    return pl.pallas_call(
        finish_kernel,
        grid=(SLOTS // STEP_HEADS,),
        in_specs=[
            pl.BlockSpec((GROUP_ROWS, STEP_HEADS * HD), lambda h: (0, h)),
            vmem,
            vmem,
            vmem,
        ],
        out_specs=[
            pl.BlockSpec((STEP_HEADS, HD, GROUP_ROWS), lambda h: (h, 0, 0)),
            pl.BlockSpec((STEP_HEADS, SLABS, PROBES), lambda h: (h, 0, 0)),
        ],
        out_shape=[
            jax.ShapeDtypeStruct((SLOTS, HD, GROUP_ROWS), jnp.bfloat16),
            jax.ShapeDtypeStruct((SLOTS, SLABS, PROBES), jnp.float32),
        ],
        name="finish",
    )(arrived, place, probe, lane)


def ring_sum(part, axis):
    size = lax.axis_size(axis)
    others = [
        lax.ppermute(part, axis, [(i, (i + step) % size) for i in range(size)])
        for step in range(1, size)
    ]
    return part + sum(others)


def body(stored, row_map, probe, lane):
    my_group = lax.axis_index(DP)
    outgoing = pack(stored).reshape(N_DP * N_MP, SUB_ROWS, SLOTS * HD)
    incoming = lax.all_to_all(outgoing, DP_MP, split_axis=0, concat_axis=0, tiled=True)
    arrived = incoming.reshape(GROUP_ROWS, SLOTS * HD)
    by_source = row_map.reshape(N_DP * N_MP, N_DP, SUB_ROWS)
    mine = lax.dynamic_index_in_dim(by_source, my_group, 1, keepdims=False)
    local_row = mine.reshape(GROUP_ROWS, 1) - my_group * GROUP_ROWS
    targets = lax.broadcasted_iota(jnp.int32, (GROUP_ROWS, GROUP_ROWS), 1)
    place = (local_row == targets).astype(jnp.bfloat16)
    shards, slab_checks = finish(arrived, place, probe, lane)
    part = jnp.sum(slab_checks, axis=1)
    for axis in reversed(DP):
        part = ring_sum(part, axis)
    return shards, slab_checks, part / (N_DP * SLABS)


def solution(mesh):
    finer = Mesh(mesh.devices.reshape(4, 4, mesh.shape["mp"]), ("dp_0", "dp_1", "mp"))
    placed = (P(DP_MP, None), P(), P(DP, None), P())
    return jax.shard_map(
        body,
        mesh=finer,
        in_specs=placed,
        out_specs=(P("mp", None, DP), P("mp", DP, None), P("mp", None)),
        check_vma=False,
    )
```

```python
import jax
import jax.numpy as jnp
from jax import lax
from jax.experimental import pallas as pl
from jax.experimental.pallas import tpu as pltpu
from jax.sharding import Mesh
from jax.sharding import PartitionSpec as P

Q_HEADS = 128
KV_HEADS = 8
HD = 128
PROBES = 1024
SLABS = 8
N_DP = 16
N_MP = 8
PER_DEVICE = Q_HEADS // N_MP
SLOTS = PER_DEVICE + 2
SUB_ROWS = 8
ROWS_DEV = 128
GROUP_ROWS = 1024
SLAB_ROWS = GROUP_ROWS // SLABS
DP = ("dp_0", "dp_1")
DP_MP = ("dp_0", "dp_1", "mp")
STEP_HEADS = 6
FETCH_HEADS = 6
PART_ROWS = STEP_HEADS * PROBES // HD
PACK_VMEM = 20 << 20
STAGE_VMEM = 8 << 20
FINISH_VMEM = 28 << 20


def in_vmem(array):
    return pltpu.with_memory_space_constraint(array, pltpu.VMEM)


def in_hbm(array):
    return pltpu.with_memory_space_constraint(array, pltpu.HBM)


def pack_kernel(stored_ref, out_ref, wide_ref, narrow_ref, in_sem, out_sem):
    query = PER_DEVICE * HD
    first_kv = Q_HEADS * HD

    def fetch(piece, start, width):
        columns = pl.ds(start, width)
        return pltpu.make_async_copy(
            stored_ref.at[:, columns], wide_ref.at[:, columns], in_sem.at[piece]
        )

    def send(m):
        return pltpu.make_async_copy(
            narrow_ref.at[m], out_ref.at[:, m], out_sem.at[m]
        )

    key_value = fetch(N_MP, first_kv, 2 * KV_HEADS * HD)
    queries = [fetch(m, m * query, query) for m in range(N_MP)]
    key_value.start()
    for copy in queries:
        copy.start()
    key_value.wait()
    for m in range(N_MP):
        key = first_kv + m * HD
        value = key + KV_HEADS * HD
        for start, width, to in ((key, HD, query), (value, HD, query + HD)):
            part = wide_ref[:, start : start + width].reshape(N_DP, SUB_ROWS, width)
            narrow_ref[m, :, :, to : to + width] = part.astype(jnp.bfloat16)
        queries[m].wait()
        part = wide_ref[:, m * query : (m + 1) * query].reshape(N_DP, SUB_ROWS, query)
        narrow_ref[m, :, :, :query] = part.astype(jnp.bfloat16)
        send(m).start()
    for m in range(N_MP):
        send(m).wait()


def pack(stored):
    return pl.pallas_call(
        pack_kernel,
        in_specs=[pl.BlockSpec(memory_space=pltpu.HBM)],
        out_specs=pl.BlockSpec(memory_space=pltpu.HBM),
        out_shape=pltpu.HBM((N_DP, N_MP, SUB_ROWS, SLOTS * HD), jnp.bfloat16),
        scratch_shapes=[
            pltpu.VMEM((ROWS_DEV, (Q_HEADS + 2 * KV_HEADS) * HD), jnp.float32),
            pltpu.VMEM((N_MP, N_DP, SUB_ROWS, SLOTS * HD), jnp.bfloat16),
            pltpu.SemaphoreType.DMA((N_MP + 1,)),
            pltpu.SemaphoreType.DMA((N_MP,)),
        ],
        compiler_params=pltpu.CompilerParams(vmem_limit_bytes=PACK_VMEM),
        name="pack",
    )(stored)


def stage_kernel(row_ref, lane_ref, place_ref, lane_out):
    targets = lax.broadcasted_iota(jnp.int32, (GROUP_ROWS, GROUP_ROWS), 1)
    place_ref[...] = jnp.where(row_ref[...] == targets, 1.0, 0.0).astype(jnp.bfloat16)
    lane_out[...] = lane_ref[...].astype(jnp.float32)


def stage(local_row, lane):
    vmem = pl.BlockSpec(memory_space=pltpu.VMEM)
    return pl.pallas_call(
        stage_kernel,
        in_specs=[vmem] * 2,
        out_specs=[vmem] * 2,
        out_shape=[
            pltpu.VMEM((GROUP_ROWS, GROUP_ROWS), jnp.bfloat16),
            pltpu.VMEM((HD, PROBES), jnp.float32),
        ],
        compiler_params=pltpu.CompilerParams(vmem_limit_bytes=STAGE_VMEM),
        cost_estimate=pl.CostEstimate(
            flops=1 << 30, bytes_accessed=8 << 20, transcendentals=0
        ),
        name="stage",
    )(local_row, in_hbm(lane))


def finish_kernel(
    arrived_hbm, place_ref, lane_ref, probe_hbm, shards_hbm, checks_hbm, part_ref,
    arrived_ref, probe_ref, shards_ref, checks_ref, in_sem, probe_sem, out_sem,
):
    width = FETCH_HEADS * HD
    fetches = SLOTS // FETCH_HEADS
    blocks = SLOTS // STEP_HEADS
    per_block = STEP_HEADS // FETCH_HEADS

    def fetch(piece):
        return pltpu.make_async_copy(
            arrived_hbm.at[:, pl.ds(pl.multiple_of(piece * width, HD), width)],
            arrived_ref.at[piece],
            in_sem.at[piece],
        )

    def send_shards(block):
        heads = pl.ds(block * STEP_HEADS, STEP_HEADS)
        return pltpu.make_async_copy(
            shards_ref.at[block], shards_hbm.at[heads], out_sem.at[0, block]
        )

    def send_checks(block):
        heads = pl.ds(block * STEP_HEADS, STEP_HEADS)
        return pltpu.make_async_copy(
            checks_ref.at[block], checks_hbm.at[heads], out_sem.at[1, block]
        )

    probe_copy = pltpu.make_async_copy(probe_hbm, probe_ref, probe_sem)
    for piece in range(per_block):
        fetch(piece).start()
    probe_copy.start()

    def one_block(block, _):
        for piece in range(per_block):
            fetch(block * per_block + piece).wait()

        @pl.when(block + 1 < blocks)
        def _():
            for piece in range(per_block):
                fetch((block + 1) * per_block + piece).start()

        for piece in range(per_block):
            placed = lax.dot_general(
                arrived_ref[block * per_block + piece],
                place_ref[...],
                (((0,), (0,)), ((), ())),
                preferred_element_type=jnp.float32,
            ).astype(jnp.bfloat16)
            first = piece * FETCH_HEADS
            shards_ref[block, first : first + FETCH_HEADS] = placed.reshape(
                FETCH_HEADS, HD, GROUP_ROWS
            )
        send_shards(block).start()

        @pl.when(block == 0)
        def _():
            probe_copy.wait()

        total = jnp.zeros((STEP_HEADS, PROBES), jnp.float32)
        for slab in range(SLABS):
            rows = slice(slab * SLAB_ROWS, (slab + 1) * SLAB_ROWS)
            projected = jnp.dot(
                shards_ref[block, :, :, rows].reshape(STEP_HEADS * HD, SLAB_ROWS),
                probe_ref[rows, :],
                preferred_element_type=jnp.float32,
            ).reshape(STEP_HEADS, HD, PROBES)
            sums = jnp.sum(projected * lane_ref[...][None], axis=1)
            checks_ref[block, :, slab, :] = sums
            total = total + sums
        part_ref[block] = total.reshape(PART_ROWS, HD).astype(jnp.bfloat16)
        send_checks(block).start()
        return 0

    lax.fori_loop(0, blocks, one_block, 0)
    for block in range(blocks):
        send_shards(block).wait()
        send_checks(block).wait()


def finish(arrived, place, lane, probe):
    vmem = pl.BlockSpec(memory_space=pltpu.VMEM)
    hbm = pl.BlockSpec(memory_space=pltpu.HBM)
    blocks = SLOTS // STEP_HEADS
    fetches = SLOTS // FETCH_HEADS
    return pl.pallas_call(
        finish_kernel,
        in_specs=[hbm, vmem, vmem, hbm],
        out_specs=[hbm, hbm, vmem],
        out_shape=[
            pltpu.HBM((SLOTS, HD, GROUP_ROWS), jnp.bfloat16),
            pltpu.HBM((SLOTS, SLABS, PROBES), jnp.float32),
            pltpu.VMEM((blocks, PART_ROWS, HD), jnp.bfloat16),
        ],
        scratch_shapes=[
            pltpu.VMEM((fetches, GROUP_ROWS, FETCH_HEADS * HD), jnp.bfloat16),
            pltpu.VMEM((GROUP_ROWS, PROBES), jnp.bfloat16),
            pltpu.VMEM((blocks, STEP_HEADS, HD, GROUP_ROWS), jnp.bfloat16),
            pltpu.VMEM((blocks, STEP_HEADS, SLABS, PROBES), jnp.float32),
            pltpu.SemaphoreType.DMA((fetches,)),
            pltpu.SemaphoreType.DMA(()),
            pltpu.SemaphoreType.DMA((2, blocks)),
        ],
        compiler_params=pltpu.CompilerParams(vmem_limit_bytes=FINISH_VMEM),
        name="finish",
    )(in_hbm(arrived), in_vmem(place), in_vmem(lane), in_hbm(probe))


def ring_sum(part, axis):
    size = lax.axis_size(axis)
    others = [
        lax.ppermute(part, axis, [(i, (i + step) % size) for i in range(size)])
        for step in (2, 1, 3)
    ]
    return sum(piece.astype(jnp.float32) for piece in [part, *others])


def body(stored, row_map, probe, lane):
    my_group = lax.axis_index(DP)
    outgoing = pack(in_hbm(stored)).reshape(N_DP * N_MP, SUB_ROWS, SLOTS * HD)
    incoming = lax.all_to_all(outgoing, DP_MP, split_axis=0, concat_axis=0, tiled=True)
    arrived = incoming.reshape(GROUP_ROWS, SLOTS * HD)
    by_source = row_map.reshape(N_DP * N_MP, N_DP, SUB_ROWS)
    mine = lax.dynamic_index_in_dim(by_source, my_group, 1, keepdims=False)
    local_row = mine.reshape(GROUP_ROWS, 1) - my_group * GROUP_ROWS
    place, lane_wide = stage(local_row, lane)
    shards, slab_checks, part = finish(arrived, place, lane_wide, probe)
    row = ring_sum(part, DP[1]).astype(jnp.bfloat16)
    total = ring_sum(row, DP[0])
    head_sums = total.reshape(SLOTS, PROBES) / (N_DP * SLABS)
    return shards, slab_checks, head_sums


def solution(mesh):
    finer = Mesh(mesh.devices.reshape(4, 4, mesh.shape["mp"]), ("dp_0", "dp_1", "mp"))
    placed = (P(DP_MP, None), P(), P(DP, None), P())
    return jax.shard_map(
        body,
        mesh=finer,
        in_specs=placed,
        out_specs=(P("mp", None, DP), P("mp", DP, None), P("mp", None)),
        check_vma=False,
    )
```

```python
import jax
import jax.numpy as jnp
from jax import lax
from jax.experimental import pallas as pl
from jax.experimental.pallas import tpu as pltpu
from jax.sharding import Mesh
from jax.sharding import PartitionSpec as P

Q_HEADS = 128
KV_HEADS = 8
HD = 128
PROBES = 1024
SLABS = 8
N_DP = 16
N_MP = 8
PER_DEVICE = Q_HEADS // N_MP
SLOTS = PER_DEVICE + 2
SUB_ROWS = 8
ROWS_DEV = 128
GROUP_ROWS = 1024
SLAB_ROWS = GROUP_ROWS // SLABS
DP = ("dp_0", "dp_1")
DP_MP = ("dp_0", "dp_1", "mp")
STEP_HEADS = 6
FETCH_HEADS = 6
PART_ROWS = STEP_HEADS * PROBES // HD
PACK_VMEM = 20 << 20
STAGE_VMEM = 8 << 20
FINISH_VMEM = 28 << 20


def in_vmem(array):
    return pltpu.with_memory_space_constraint(array, pltpu.VMEM)


def in_hbm(array):
    return pltpu.with_memory_space_constraint(array, pltpu.HBM)


def pack_kernel(stored_ref, out_ref, wide_ref, narrow_ref, in_sem, out_sem):
    query = PER_DEVICE * HD
    first_kv = Q_HEADS * HD

    def fetch(piece, start, width):
        columns = pl.ds(start, width)
        return pltpu.make_async_copy(
            stored_ref.at[:, columns], wide_ref.at[:, columns], in_sem.at[piece]
        )

    def send(m):
        return pltpu.make_async_copy(
            narrow_ref.at[m], out_ref.at[:, m], out_sem.at[m]
        )

    key_value = fetch(N_MP, first_kv, 2 * KV_HEADS * HD)
    queries = [fetch(m, m * query, query) for m in range(N_MP)]
    key_value.start()
    for copy in queries:
        copy.start()
    key_value.wait()
    for m in range(N_MP):
        key = first_kv + m * HD
        value = key + KV_HEADS * HD
        for start, width, to in ((key, HD, query), (value, HD, query + HD)):
            part = wide_ref[:, start : start + width].reshape(N_DP, SUB_ROWS, width)
            narrow_ref[m, :, :, to : to + width] = part.astype(jnp.bfloat16)
        queries[m].wait()
        part = wide_ref[:, m * query : (m + 1) * query].reshape(N_DP, SUB_ROWS, query)
        narrow_ref[m, :, :, :query] = part.astype(jnp.bfloat16)
        send(m).start()
    for m in range(N_MP):
        send(m).wait()


def pack(stored):
    return pl.pallas_call(
        pack_kernel,
        in_specs=[pl.BlockSpec(memory_space=pltpu.HBM)],
        out_specs=pl.BlockSpec(memory_space=pltpu.HBM),
        out_shape=pltpu.HBM((N_DP, N_MP, SUB_ROWS, SLOTS * HD), jnp.bfloat16),
        scratch_shapes=[
            pltpu.VMEM((ROWS_DEV, (Q_HEADS + 2 * KV_HEADS) * HD), jnp.float32),
            pltpu.VMEM((N_MP, N_DP, SUB_ROWS, SLOTS * HD), jnp.bfloat16),
            pltpu.SemaphoreType.DMA((N_MP + 1,)),
            pltpu.SemaphoreType.DMA((N_MP,)),
        ],
        compiler_params=pltpu.CompilerParams(vmem_limit_bytes=PACK_VMEM),
        name="pack",
    )(stored)


def stage_kernel(row_ref, lane_ref, place_ref, lane_out):
    targets = lax.broadcasted_iota(jnp.int32, (GROUP_ROWS, GROUP_ROWS), 1)
    place_ref[...] = jnp.where(row_ref[...] == targets, 1.0, 0.0).astype(jnp.bfloat16)
    lane_out[...] = lane_ref[...].astype(jnp.float32)


def stage(local_row, lane):
    vmem = pl.BlockSpec(memory_space=pltpu.VMEM)
    return pl.pallas_call(
        stage_kernel,
        in_specs=[vmem] * 2,
        out_specs=[vmem] * 2,
        out_shape=[
            pltpu.VMEM((GROUP_ROWS, GROUP_ROWS), jnp.bfloat16),
            pltpu.VMEM((HD, PROBES), jnp.float32),
        ],
        compiler_params=pltpu.CompilerParams(vmem_limit_bytes=STAGE_VMEM),
        cost_estimate=pl.CostEstimate(
            flops=1 << 30, bytes_accessed=8 << 20, transcendentals=0
        ),
        name="stage",
    )(local_row, in_hbm(lane))


def finish_kernel(
    arrived_hbm, place_ref, lane_ref, probe_hbm, shards_hbm, checks_hbm, part_ref,
    arrived_ref, probe_ref, shards_ref, checks_ref, in_sem, probe_sem, out_sem,
):
    width = FETCH_HEADS * HD
    fetches = SLOTS // FETCH_HEADS
    blocks = SLOTS // STEP_HEADS
    per_block = STEP_HEADS // FETCH_HEADS

    def fetch(piece):
        return pltpu.make_async_copy(
            arrived_hbm.at[:, pl.ds(pl.multiple_of(piece * width, HD), width)],
            arrived_ref.at[piece],
            in_sem.at[piece],
        )

    def send_shards(block):
        heads = pl.ds(block * STEP_HEADS, STEP_HEADS)
        return pltpu.make_async_copy(
            shards_ref.at[block], shards_hbm.at[heads], out_sem.at[0, block]
        )

    def send_checks(block):
        heads = pl.ds(block * STEP_HEADS, STEP_HEADS)
        return pltpu.make_async_copy(
            checks_ref.at[block], checks_hbm.at[heads], out_sem.at[1, block]
        )

    probe_copy = pltpu.make_async_copy(probe_hbm, probe_ref, probe_sem)
    for piece in range(per_block):
        fetch(piece).start()
    probe_copy.start()

    def one_block(block, _):
        for piece in range(per_block):
            fetch(block * per_block + piece).wait()

        @pl.when(block + 1 < blocks)
        def _():
            for piece in range(per_block):
                fetch((block + 1) * per_block + piece).start()

        for piece in range(per_block):
            placed = lax.dot_general(
                arrived_ref[block * per_block + piece],
                place_ref[...],
                (((0,), (0,)), ((), ())),
                preferred_element_type=jnp.float32,
            ).astype(jnp.bfloat16)
            first = piece * FETCH_HEADS
            shards_ref[block, first : first + FETCH_HEADS] = placed.reshape(
                FETCH_HEADS, HD, GROUP_ROWS
            )
        send_shards(block).start()

        @pl.when(block == 0)
        def _():
            probe_copy.wait()

        total = jnp.zeros((STEP_HEADS, PROBES), jnp.float32)
        for slab in range(SLABS):
            rows = slice(slab * SLAB_ROWS, (slab + 1) * SLAB_ROWS)
            projected = jnp.dot(
                shards_ref[block, :, :, rows].reshape(STEP_HEADS * HD, SLAB_ROWS),
                probe_ref[rows, :],
                preferred_element_type=jnp.float32,
            ).reshape(STEP_HEADS, HD, PROBES)
            sums = jnp.sum(projected * lane_ref[...][None], axis=1)
            checks_ref[block, :, slab, :] = sums
            total = total + sums
        part_ref[block] = total.reshape(PART_ROWS, HD)
        send_checks(block).start()
        return 0

    lax.fori_loop(0, blocks, one_block, 0)
    for block in range(blocks):
        send_shards(block).wait()
        send_checks(block).wait()


def finish(arrived, place, lane, probe):
    vmem = pl.BlockSpec(memory_space=pltpu.VMEM)
    hbm = pl.BlockSpec(memory_space=pltpu.HBM)
    blocks = SLOTS // STEP_HEADS
    fetches = SLOTS // FETCH_HEADS
    return pl.pallas_call(
        finish_kernel,
        in_specs=[hbm, vmem, vmem, hbm],
        out_specs=[hbm, hbm, vmem],
        out_shape=[
            pltpu.HBM((SLOTS, HD, GROUP_ROWS), jnp.bfloat16),
            pltpu.HBM((SLOTS, SLABS, PROBES), jnp.float32),
            pltpu.VMEM((blocks, PART_ROWS, HD), jnp.float32),
        ],
        scratch_shapes=[
            pltpu.VMEM((fetches, GROUP_ROWS, FETCH_HEADS * HD), jnp.bfloat16),
            pltpu.VMEM((GROUP_ROWS, PROBES), jnp.bfloat16),
            pltpu.VMEM((blocks, STEP_HEADS, HD, GROUP_ROWS), jnp.bfloat16),
            pltpu.VMEM((blocks, STEP_HEADS, SLABS, PROBES), jnp.float32),
            pltpu.SemaphoreType.DMA((fetches,)),
            pltpu.SemaphoreType.DMA(()),
            pltpu.SemaphoreType.DMA((2, blocks)),
        ],
        compiler_params=pltpu.CompilerParams(vmem_limit_bytes=FINISH_VMEM),
        name="finish",
    )(in_hbm(arrived), in_vmem(place), in_vmem(lane), in_hbm(probe))


def ring_sum(part, axis):
    size = lax.axis_size(axis)
    others = [
        lax.ppermute(part, axis, [(i, (i + step) % size) for i in range(size)])
        for step in (3, 2, 1)
    ]
    return sum([part, *others])


def body(stored, row_map, probe, lane):
    my_group = lax.axis_index(DP)
    outgoing = pack(in_hbm(stored)).reshape(N_DP * N_MP, SUB_ROWS, SLOTS * HD)
    incoming = lax.all_to_all(outgoing, DP_MP, split_axis=0, concat_axis=0, tiled=True)
    arrived = incoming.reshape(GROUP_ROWS, SLOTS * HD)
    by_source = row_map.reshape(N_DP * N_MP, N_DP, SUB_ROWS)
    mine = lax.dynamic_index_in_dim(by_source, my_group, 1, keepdims=False)
    local_row = mine.reshape(GROUP_ROWS, 1) - my_group * GROUP_ROWS
    place, lane_wide = stage(local_row, lane)
    shards, slab_checks, part = finish(arrived, place, lane_wide, probe)
    row = ring_sum(part, DP[1])
    total = ring_sum(row, DP[0])
    head_sums = total.reshape(SLOTS, PROBES) / (N_DP * SLABS)
    return shards, slab_checks, head_sums


def solution(mesh):
    finer = Mesh(mesh.devices.reshape(4, 4, mesh.shape["mp"]), ("dp_0", "dp_1", "mp"))
    placed = (P(DP_MP, None), P(), P(DP, None), P())
    return jax.shard_map(
        body,
        mesh=finer,
        in_specs=placed,
        out_specs=(P("mp", None, DP), P("mp", DP, None), P("mp", None)),
        check_vma=False,
    )
```

```python
import jax
import jax.numpy as jnp
from jax import lax
from jax.experimental import pallas as pl
from jax.experimental.pallas import tpu as pltpu
from jax.sharding import Mesh
from jax.sharding import PartitionSpec as P

Q_HEADS = 128
KV_HEADS = 8
HD = 128
PROBES = 1024
SLABS = 8
N_DP = 16
N_MP = 8
PER_DEVICE = Q_HEADS // N_MP
SLOTS = PER_DEVICE + 2
SUB_ROWS = 8
ROWS_DEV = 128
GROUP_ROWS = 1024
SLAB_ROWS = GROUP_ROWS // SLABS
DP = ("dp_0", "dp_1")
MP = ("mp_0", "mp_1")
DP_MP = DP + MP
EXCHANGE = ("mp_0", "mp_1", "dp_1", "dp_0")
SIDE = 4
STEP_HEADS = 6
FETCH_HEADS = 6
PART_ROWS = STEP_HEADS * PROBES // HD
PACK_VMEM = 20 << 20
STAGE_VMEM = 8 << 20
FINISH_VMEM = 28 << 20


def in_vmem(array):
    return pltpu.with_memory_space_constraint(array, pltpu.VMEM)


def in_hbm(array):
    return pltpu.with_memory_space_constraint(array, pltpu.HBM)


def pack_kernel(stored_ref, out_ref, wide_ref, narrow_ref, in_sem, out_sem):
    query = PER_DEVICE * HD
    first_kv = Q_HEADS * HD

    def fetch(piece, start, width):
        columns = pl.ds(start, width)
        return pltpu.make_async_copy(
            stored_ref.at[:, columns], wide_ref.at[:, columns], in_sem.at[piece]
        )

    def send(m):
        return pltpu.make_async_copy(
            narrow_ref.at[m], out_ref.at[m], out_sem.at[m]
        )

    key_value = fetch(N_MP, first_kv, 2 * KV_HEADS * HD)
    queries = [fetch(m, m * query, query) for m in range(N_MP)]
    key_value.start()
    for copy in queries:
        copy.start()
    key_value.wait()
    def place(m, start, width, to):
        for y in range(SIDE):
            for x in range(SIDE):
                first = (y * SIDE + x) * SUB_ROWS
                part = wide_ref[first : first + SUB_ROWS, start : start + width]
                narrow_ref[m, x * SIDE + y, :, to : to + width] = part.astype(
                    jnp.bfloat16
                )

    for m in range(N_MP):
        key = first_kv + m * HD
        place(m, key, HD, query)
        place(m, key + KV_HEADS * HD, HD, query + HD)
        queries[m].wait()
        place(m, m * query, query, 0)
        send(m).start()
    for m in range(N_MP):
        send(m).wait()


def pack(stored):
    return pl.pallas_call(
        pack_kernel,
        in_specs=[pl.BlockSpec(memory_space=pltpu.HBM)],
        out_specs=pl.BlockSpec(memory_space=pltpu.HBM),
        out_shape=pltpu.HBM((N_MP, N_DP, SUB_ROWS, SLOTS * HD), jnp.bfloat16),
        scratch_shapes=[
            pltpu.VMEM((ROWS_DEV, (Q_HEADS + 2 * KV_HEADS) * HD), jnp.float32),
            pltpu.VMEM((N_MP, N_DP, SUB_ROWS, SLOTS * HD), jnp.bfloat16),
            pltpu.SemaphoreType.DMA((N_MP + 1,)),
            pltpu.SemaphoreType.DMA((N_MP,)),
        ],
        compiler_params=pltpu.CompilerParams(vmem_limit_bytes=PACK_VMEM),
        name="pack",
    )(stored)


def stage_kernel(row_ref, lane_ref, place_ref, lane_out):
    targets = lax.broadcasted_iota(jnp.int32, (GROUP_ROWS, GROUP_ROWS), 1)
    place_ref[...] = jnp.where(row_ref[...] == targets, 1.0, 0.0).astype(jnp.bfloat16)
    lane_out[...] = lane_ref[...].astype(jnp.float32)


def stage(local_row, lane):
    vmem = pl.BlockSpec(memory_space=pltpu.VMEM)
    return pl.pallas_call(
        stage_kernel,
        in_specs=[vmem] * 2,
        out_specs=[vmem] * 2,
        out_shape=[
            pltpu.VMEM((GROUP_ROWS, GROUP_ROWS), jnp.bfloat16),
            pltpu.VMEM((HD, PROBES), jnp.float32),
        ],
        compiler_params=pltpu.CompilerParams(vmem_limit_bytes=STAGE_VMEM),
        cost_estimate=pl.CostEstimate(
            flops=1 << 30, bytes_accessed=8 << 20, transcendentals=0
        ),
        name="stage",
    )(local_row, in_hbm(lane))


def finish_kernel(
    arrived_hbm, place_ref, lane_ref, probe_hbm, shards_hbm, checks_ref, part_ref,
    arrived_ref, probe_ref, shards_ref, in_sem, probe_sem, out_sem,
):
    width = FETCH_HEADS * HD
    fetches = SLOTS // FETCH_HEADS
    blocks = SLOTS // STEP_HEADS
    per_block = STEP_HEADS // FETCH_HEADS

    def fetch(piece):
        return pltpu.make_async_copy(
            arrived_hbm.at[:, pl.ds(pl.multiple_of(piece * width, HD), width)],
            arrived_ref.at[piece],
            in_sem.at[piece],
        )

    def send_shards(block):
        heads = pl.ds(block * STEP_HEADS, STEP_HEADS)
        return pltpu.make_async_copy(
            shards_ref.at[block], shards_hbm.at[heads], out_sem.at[block]
        )

    probe_copy = pltpu.make_async_copy(probe_hbm, probe_ref, probe_sem)
    for piece in range(per_block):
        fetch(piece).start()
    probe_copy.start()

    def one_block(block, _):
        for piece in range(per_block):
            fetch(block * per_block + piece).wait()

        @pl.when(block + 1 < blocks)
        def _():
            for piece in range(per_block):
                fetch((block + 1) * per_block + piece).start()

        for piece in range(per_block):
            placed = lax.dot_general(
                arrived_ref[block * per_block + piece],
                place_ref[...],
                (((0,), (0,)), ((), ())),
                preferred_element_type=jnp.float32,
            ).astype(jnp.bfloat16)
            first = piece * FETCH_HEADS
            shards_ref[block, first : first + FETCH_HEADS] = placed.reshape(
                FETCH_HEADS, HD, GROUP_ROWS
            )
        send_shards(block).start()

        @pl.when(block == 0)
        def _():
            probe_copy.wait()

        heads = pl.ds(block * STEP_HEADS, STEP_HEADS)
        total = jnp.zeros((STEP_HEADS, PROBES), jnp.float32)
        for slab in range(SLABS):
            rows = slice(slab * SLAB_ROWS, (slab + 1) * SLAB_ROWS)
            projected = jnp.dot(
                shards_ref[block, :, :, rows].reshape(STEP_HEADS * HD, SLAB_ROWS),
                probe_ref[rows, :],
                preferred_element_type=jnp.float32,
            ).reshape(STEP_HEADS, HD, PROBES)
            sums = jnp.sum(projected * lane_ref[...][None], axis=1)
            checks_ref[heads, slab, :] = sums
            total = total + sums
        part_ref[block] = total.reshape(PART_ROWS, HD)
        return 0

    lax.fori_loop(0, blocks, one_block, 0)
    for block in range(blocks):
        send_shards(block).wait()


def finish(arrived, place, lane, probe):
    vmem = pl.BlockSpec(memory_space=pltpu.VMEM)
    hbm = pl.BlockSpec(memory_space=pltpu.HBM)
    blocks = SLOTS // STEP_HEADS
    fetches = SLOTS // FETCH_HEADS
    return pl.pallas_call(
        finish_kernel,
        in_specs=[hbm, vmem, vmem, hbm],
        out_specs=[hbm, vmem, vmem],
        out_shape=[
            pltpu.HBM((SLOTS, HD, GROUP_ROWS), jnp.bfloat16),
            pltpu.VMEM((SLOTS, SLABS, PROBES), jnp.float32),
            pltpu.VMEM((blocks, PART_ROWS, HD), jnp.float32),
        ],
        scratch_shapes=[
            pltpu.VMEM((fetches, GROUP_ROWS, FETCH_HEADS * HD), jnp.bfloat16),
            pltpu.VMEM((GROUP_ROWS, PROBES), jnp.bfloat16),
            pltpu.VMEM((blocks, STEP_HEADS, HD, GROUP_ROWS), jnp.bfloat16),
            pltpu.SemaphoreType.DMA((fetches,)),
            pltpu.SemaphoreType.DMA(()),
            pltpu.SemaphoreType.DMA((blocks,)),
        ],
        compiler_params=pltpu.CompilerParams(vmem_limit_bytes=FINISH_VMEM),
        name="finish",
    )(in_hbm(arrived), in_vmem(place), in_vmem(lane), in_hbm(probe))


def ring_sum(part, axis):
    size = lax.axis_size(axis)
    others = [
        lax.ppermute(part, axis, [(i, (i + step) % size) for i in range(size)])
        for step in (3, 1, 2)
    ]
    return sum([part, *others])


def body(stored, row_map, probe, lane):
    my_group = lax.axis_index(DP)
    outgoing = pack(in_hbm(stored)).reshape(N_DP * N_MP, SUB_ROWS, SLOTS * HD)
    incoming = lax.all_to_all(outgoing, EXCHANGE, split_axis=0, concat_axis=0, tiled=True)
    arrived = incoming.reshape(GROUP_ROWS, SLOTS * HD)
    by_source = row_map.reshape(N_DP * N_MP, N_DP, SUB_ROWS)
    mine = lax.dynamic_index_in_dim(by_source, my_group, 1, keepdims=False)
    mine = mine.reshape(SIDE, SIDE, N_MP, SUB_ROWS).transpose(2, 1, 0, 3)
    local_row = mine.reshape(GROUP_ROWS, 1) - my_group * GROUP_ROWS
    place, lane_wide = stage(local_row, lane)
    shards, slab_checks, part = finish(arrived, place, lane_wide, probe)
    row = ring_sum(part, DP[1])
    total = ring_sum(row, DP[0])
    head_sums = total.reshape(SLOTS, PROBES) / (N_DP * SLABS)
    return shards, slab_checks, head_sums


def solution(mesh):
    finer = Mesh(mesh.devices.reshape(SIDE, SIDE, SIDE, 2), DP_MP)
    placed = (P(DP_MP, None), P(), P(DP, None), P())
    return jax.shard_map(
        body,
        mesh=finer,
        in_specs=placed,
        out_specs=(P(MP, None, DP), P(MP, DP, None), P(MP, None)),
        check_vma=False,
    )
```

```python
import jax
import jax.numpy as jnp
from jax import lax
from jax.experimental import pallas as pl
from jax.experimental.pallas import tpu as pltpu
from jax.sharding import Mesh
from jax.sharding import PartitionSpec as P

Q_HEADS = 128
KV_HEADS = 8
HD = 128
PROBES = 1024
SLABS = 8
N_DP = 16
N_MP = 8
PER_DEVICE = Q_HEADS // N_MP
SLOTS = PER_DEVICE + 2
SUB_ROWS = 8
ROWS_DEV = 128
GROUP_ROWS = 1024
SLAB_ROWS = GROUP_ROWS // SLABS
DP = ("dp_0", "dp_1")
MP = ("mp_0", "mp_1")
DP_MP = DP + MP
EXCHANGE = ("mp_0", "mp_1", "dp_1", "dp_0")
SIDE = 4
STEP_HEADS = 6
FETCH_HEADS = 2
PART_ROWS = STEP_HEADS * PROBES // HD
PACK_VMEM = 20 << 20
STAGE_VMEM = 8 << 20
FINISH_VMEM = 28 << 20


def in_vmem(array):
    return pltpu.with_memory_space_constraint(array, pltpu.VMEM)


def in_hbm(array):
    return pltpu.with_memory_space_constraint(array, pltpu.HBM)


def pack_kernel(stored_ref, out_ref, wide_ref, narrow_ref, in_sem, out_sem):
    query = PER_DEVICE * HD
    first_kv = Q_HEADS * HD

    def fetch(piece, start, width):
        columns = pl.ds(start, width)
        return pltpu.make_async_copy(
            stored_ref.at[:, columns], wide_ref.at[:, columns], in_sem.at[piece]
        )

    def send(m):
        return pltpu.make_async_copy(
            narrow_ref.at[m], out_ref.at[m], out_sem.at[m]
        )

    key_value = fetch(N_MP, first_kv, 2 * KV_HEADS * HD)
    queries = [fetch(m, m * query, query) for m in range(N_MP)]
    key_value.start()
    for copy in queries:
        copy.start()
    key_value.wait()
    def place(m, start, width, to):
        for y in range(SIDE):
            for x in range(SIDE):
                first = (y * SIDE + x) * SUB_ROWS
                part = wide_ref[first : first + SUB_ROWS, start : start + width]
                narrow_ref[m, x * SIDE + y, :, to : to + width] = part.astype(
                    jnp.bfloat16
                )

    for m in range(N_MP):
        key = first_kv + m * HD
        place(m, key, HD, query)
        place(m, key + KV_HEADS * HD, HD, query + HD)
        queries[m].wait()
        place(m, m * query, query, 0)
        send(m).start()
    for m in range(N_MP):
        send(m).wait()


def pack(stored):
    return pl.pallas_call(
        pack_kernel,
        in_specs=[pl.BlockSpec(memory_space=pltpu.HBM)],
        out_specs=pl.BlockSpec(memory_space=pltpu.HBM),
        out_shape=pltpu.HBM((N_MP, N_DP, SUB_ROWS, SLOTS * HD), jnp.bfloat16),
        scratch_shapes=[
            pltpu.VMEM((ROWS_DEV, (Q_HEADS + 2 * KV_HEADS) * HD), jnp.float32),
            pltpu.VMEM((N_MP, N_DP, SUB_ROWS, SLOTS * HD), jnp.bfloat16),
            pltpu.SemaphoreType.DMA((N_MP + 1,)),
            pltpu.SemaphoreType.DMA((N_MP,)),
        ],
        compiler_params=pltpu.CompilerParams(vmem_limit_bytes=PACK_VMEM),
        name="pack",
    )(stored)


def stage_kernel(row_ref, lane_ref, place_ref, lane_out):
    targets = lax.broadcasted_iota(jnp.int32, (GROUP_ROWS, GROUP_ROWS), 1)
    place_ref[...] = jnp.where(row_ref[...] == targets, 1.0, 0.0).astype(jnp.bfloat16)
    lane_out[...] = lane_ref[...].astype(jnp.float32)


def stage(local_row, lane):
    vmem = pl.BlockSpec(memory_space=pltpu.VMEM)
    return pl.pallas_call(
        stage_kernel,
        in_specs=[vmem] * 2,
        out_specs=[vmem] * 2,
        out_shape=[
            pltpu.VMEM((GROUP_ROWS, GROUP_ROWS), jnp.bfloat16),
            pltpu.VMEM((HD, PROBES), jnp.float32),
        ],
        compiler_params=pltpu.CompilerParams(vmem_limit_bytes=STAGE_VMEM),
        cost_estimate=pl.CostEstimate(
            flops=1 << 30, bytes_accessed=8 << 20, transcendentals=0
        ),
        name="stage",
    )(local_row, in_hbm(lane))


def finish_kernel(
    arrived_hbm, place_ref, lane_ref, probe_hbm, shards_hbm, checks_ref, part_ref,
    arrived_ref, probe_ref, shards_ref, flipped_ref, in_sem, probe_sem, out_sem,
):
    width = FETCH_HEADS * HD
    fetches = SLOTS // FETCH_HEADS
    blocks = SLOTS // STEP_HEADS
    per_block = STEP_HEADS // FETCH_HEADS

    def fetch(piece):
        return pltpu.make_async_copy(
            arrived_hbm.at[:, pl.ds(piece * width, width)],
            arrived_ref.at[piece],
            in_sem.at[piece],
        )

    def send_shards(block):
        heads = pl.ds(block * STEP_HEADS, STEP_HEADS)
        return pltpu.make_async_copy(
            shards_ref.at[block], shards_hbm.at[heads], out_sem.at[block]
        )

    def flip(block, piece):
        rows = slice(piece * width, (piece + 1) * width)
        flipped_ref[block % 2, rows] = arrived_ref[block * per_block + piece].T

    probe_copy = pltpu.make_async_copy(probe_hbm, probe_ref, probe_sem)
    for piece in range(per_block):
        fetch(piece).start()
    probe_copy.start()
    for piece in range(per_block, fetches):
        fetch(piece).start()
    for piece in range(per_block):
        fetch(piece).wait()
        flip(0, piece)
    for block in range(blocks):
        placed = jnp.dot(
            flipped_ref[block % 2], place_ref[...], preferred_element_type=jnp.float32
        ).astype(jnp.bfloat16)
        shards_ref[block] = placed.reshape(STEP_HEADS, HD, GROUP_ROWS)
        send_shards(block).start()
        if block == 0:
            probe_copy.wait()
            for piece in range(per_block, fetches):
                fetch(piece).wait()
        total = jnp.zeros((STEP_HEADS, PROBES), jnp.float32)
        heads = slice(block * STEP_HEADS, (block + 1) * STEP_HEADS)
        for slab in range(SLABS):
            rows = slice(slab * SLAB_ROWS, (slab + 1) * SLAB_ROWS)
            projected = jnp.dot(
                shards_ref[block, :, :, rows].reshape(STEP_HEADS * HD, SLAB_ROWS),
                probe_ref[rows, :],
                preferred_element_type=jnp.float32,
            ).reshape(STEP_HEADS, HD, PROBES)
            sums = jnp.sum(projected * lane_ref[...][None], axis=1)
            checks_ref[heads, slab, :] = sums
            total = total + sums
            if block + 1 < blocks and slab < per_block:
                flip(block + 1, slab)
        part_ref[block] = total.reshape(PART_ROWS, HD)
    for block in range(blocks):
        send_shards(block).wait()


def finish(arrived, place, lane, probe):
    vmem = pl.BlockSpec(memory_space=pltpu.VMEM)
    hbm = pl.BlockSpec(memory_space=pltpu.HBM)
    blocks = SLOTS // STEP_HEADS
    fetches = SLOTS // FETCH_HEADS
    return pl.pallas_call(
        finish_kernel,
        in_specs=[hbm, vmem, vmem, hbm],
        out_specs=[hbm, vmem, vmem],
        out_shape=[
            pltpu.HBM((SLOTS, HD, GROUP_ROWS), jnp.bfloat16),
            pltpu.VMEM((SLOTS, SLABS, PROBES), jnp.float32),
            pltpu.VMEM((blocks, PART_ROWS, HD), jnp.float32),
        ],
        scratch_shapes=[
            pltpu.VMEM((fetches, GROUP_ROWS, FETCH_HEADS * HD), jnp.bfloat16),
            pltpu.VMEM((GROUP_ROWS, PROBES), jnp.bfloat16),
            pltpu.VMEM((blocks, STEP_HEADS, HD, GROUP_ROWS), jnp.bfloat16),
            pltpu.VMEM((2, STEP_HEADS * HD, GROUP_ROWS), jnp.bfloat16),
            pltpu.SemaphoreType.DMA((fetches,)),
            pltpu.SemaphoreType.DMA(()),
            pltpu.SemaphoreType.DMA((blocks,)),
        ],
        compiler_params=pltpu.CompilerParams(vmem_limit_bytes=FINISH_VMEM),
        name="finish",
    )(in_hbm(arrived), in_vmem(place), in_vmem(lane), in_hbm(probe))


def ring_sum(part, axis):
    size = lax.axis_size(axis)
    others = [
        lax.ppermute(part, axis, [(i, (i + step) % size) for i in range(size)])
        for step in (3, 1, 2)
    ]
    return sum([part, *others])


def body(stored, row_map, probe, lane):
    my_group = lax.axis_index(DP)
    outgoing = pack(in_hbm(stored)).reshape(N_DP * N_MP, SUB_ROWS, SLOTS * HD)
    incoming = lax.all_to_all(outgoing, EXCHANGE, split_axis=0, concat_axis=0, tiled=True)
    arrived = incoming.reshape(GROUP_ROWS, SLOTS * HD)
    by_source = row_map.reshape(N_DP * N_MP, N_DP, SUB_ROWS)
    mine = lax.dynamic_index_in_dim(by_source, my_group, 1, keepdims=False)
    mine = mine.reshape(SIDE, SIDE, N_MP, SUB_ROWS).transpose(2, 1, 0, 3)
    local_row = mine.reshape(GROUP_ROWS, 1) - my_group * GROUP_ROWS
    place, lane_wide = stage(local_row, lane)
    shards, slab_checks, part = finish(arrived, place, lane_wide, probe)
    row = ring_sum(part, DP[1])
    total = ring_sum(row, DP[0])
    head_sums = total.reshape(SLOTS, PROBES) / (N_DP * SLABS)
    return shards, slab_checks, head_sums


def solution(mesh):
    finer = Mesh(mesh.devices.reshape(SIDE, SIDE, SIDE, 2), DP_MP)
    placed = (P(DP_MP, None), P(), P(DP, None), P())
    return jax.shard_map(
        body,
        mesh=finer,
        in_specs=placed,
        out_specs=(P(MP, None, DP), P(MP, DP, None), P(MP, None)),
        check_vma=False,
    )
```

```python
import jax
import jax.numpy as jnp
from jax import lax
from jax.experimental import pallas as pl
from jax.experimental.pallas import tpu as pltpu
from jax.sharding import Mesh
from jax.sharding import PartitionSpec as P

Q_HEADS = 128
KV_HEADS = 8
HD = 128
PROBES = 1024
SLABS = 8
N_DP = 16
N_MP = 8
PER_DEVICE = Q_HEADS // N_MP
SLOTS = PER_DEVICE + 2
SUB_ROWS = 8
ROWS_DEV = 128
GROUP_ROWS = 1024
SLAB_ROWS = GROUP_ROWS // SLABS
DP = ("dp_0", "dp_1")
MP = ("mp_0", "mp_1")
DP_MP = DP + MP
EXCHANGE = ("mp_0", "mp_1", "dp_1", "dp_0")
SIDE = 4
STEP_HEADS = 6
FETCH_HEADS = 2
PART_ROWS = STEP_HEADS * PROBES // HD
PACK_VMEM = 20 << 20
STAGE_VMEM = 8 << 20
FINISH_VMEM = 28 << 20


def in_vmem(array):
    return pltpu.with_memory_space_constraint(array, pltpu.VMEM)


def in_hbm(array):
    return pltpu.with_memory_space_constraint(array, pltpu.HBM)


def pack_kernel(stored_ref, out_ref, wide_ref, narrow_ref, in_sem, out_sem):
    query = PER_DEVICE * HD
    first_kv = Q_HEADS * HD

    def fetch(piece, start, width):
        columns = pl.ds(start, width)
        return pltpu.make_async_copy(
            stored_ref.at[:, columns], wide_ref.at[:, columns], in_sem.at[piece]
        )

    def send(m):
        return pltpu.make_async_copy(
            narrow_ref.at[m], out_ref.at[m], out_sem.at[m]
        )

    key_value = fetch(N_MP, first_kv, 2 * KV_HEADS * HD)
    queries = [fetch(m, m * query, query) for m in range(N_MP)]
    key_value.start()
    for copy in queries:
        copy.start()
    key_value.wait()
    def place(m, start, width, to):
        for y in range(SIDE):
            for x in range(SIDE):
                first = (y * SIDE + x) * SUB_ROWS
                part = wide_ref[first : first + SUB_ROWS, start : start + width]
                narrow_ref[m, x * SIDE + y, :, to : to + width] = part.astype(
                    jnp.bfloat16
                )

    for m in range(N_MP):
        key = first_kv + m * HD
        place(m, key, HD, query)
        place(m, key + KV_HEADS * HD, HD, query + HD)
        queries[m].wait()
        place(m, m * query, query, 0)
        send(m).start()
    for m in range(N_MP):
        send(m).wait()


def pack(stored):
    return pl.pallas_call(
        pack_kernel,
        in_specs=[pl.BlockSpec(memory_space=pltpu.HBM)],
        out_specs=pl.BlockSpec(memory_space=pltpu.HBM),
        out_shape=pltpu.HBM((N_MP, N_DP, SUB_ROWS, SLOTS * HD), jnp.bfloat16),
        scratch_shapes=[
            pltpu.VMEM((ROWS_DEV, (Q_HEADS + 2 * KV_HEADS) * HD), jnp.float32),
            pltpu.VMEM((N_MP, N_DP, SUB_ROWS, SLOTS * HD), jnp.bfloat16),
            pltpu.SemaphoreType.DMA((N_MP + 1,)),
            pltpu.SemaphoreType.DMA((N_MP,)),
        ],
        compiler_params=pltpu.CompilerParams(vmem_limit_bytes=PACK_VMEM),
        name="pack",
    )(stored)


def stage_kernel(row_ref, lane_ref, place_ref, lane_out):
    targets = lax.broadcasted_iota(jnp.int32, (GROUP_ROWS, GROUP_ROWS), 1)
    place_ref[...] = jnp.where(row_ref[...] == targets, 1.0, 0.0).astype(jnp.bfloat16)
    lane_out[...] = lane_ref[...].astype(jnp.float32)


def stage(local_row, lane):
    vmem = pl.BlockSpec(memory_space=pltpu.VMEM)
    return pl.pallas_call(
        stage_kernel,
        in_specs=[vmem] * 2,
        out_specs=[vmem] * 2,
        out_shape=[
            pltpu.VMEM((GROUP_ROWS, GROUP_ROWS), jnp.bfloat16),
            pltpu.VMEM((HD, PROBES), jnp.float32),
        ],
        compiler_params=pltpu.CompilerParams(vmem_limit_bytes=STAGE_VMEM),
        cost_estimate=pl.CostEstimate(
            flops=1 << 30, bytes_accessed=8 << 20, transcendentals=0
        ),
        name="stage",
    )(local_row, in_hbm(lane))


def finish_kernel(
    arrived_hbm, place_ref, lane_ref, probe_hbm, shards_hbm, checks_ref, part_ref,
    arrived_ref, probe_ref, shards_ref, flipped_ref, in_sem, probe_sem, out_sem,
):
    width = FETCH_HEADS * HD
    fetches = SLOTS // FETCH_HEADS
    blocks = SLOTS // STEP_HEADS
    per_block = STEP_HEADS // FETCH_HEADS

    def fetch(piece):
        return pltpu.make_async_copy(
            arrived_hbm.at[:, pl.ds(piece * width, width)],
            arrived_ref.at[piece],
            in_sem.at[piece],
        )

    def send_shards(block):
        heads = pl.ds(block * STEP_HEADS, STEP_HEADS)
        return pltpu.make_async_copy(
            shards_ref.at[block], shards_hbm.at[heads], out_sem.at[block]
        )

    def flip(block, piece):
        rows = slice(piece * width, (piece + 1) * width)
        flipped_ref[block % 2, rows] = arrived_ref[block * per_block + piece].T

    probe_copy = pltpu.make_async_copy(probe_hbm, probe_ref, probe_sem)
    for piece in range(per_block):
        fetch(piece).start()
    probe_copy.start()
    for piece in range(per_block):
        fetch(piece).wait()
        if piece == 0:
            for later in range(per_block, fetches):
                fetch(later).start()
        flip(0, piece)
    for block in range(blocks):
        placed = jnp.dot(
            flipped_ref[block % 2], place_ref[...], preferred_element_type=jnp.float32
        ).astype(jnp.bfloat16)
        shards_ref[block] = placed.reshape(STEP_HEADS, HD, GROUP_ROWS)
        send_shards(block).start()
        if block == 0:
            probe_copy.wait()
            for piece in range(per_block, fetches):
                fetch(piece).wait()
        total = jnp.zeros((STEP_HEADS, PROBES), jnp.float32)
        heads = slice(block * STEP_HEADS, (block + 1) * STEP_HEADS)
        for slab in range(SLABS):
            rows = slice(slab * SLAB_ROWS, (slab + 1) * SLAB_ROWS)
            projected = jnp.dot(
                shards_ref[block, :, :, rows].reshape(STEP_HEADS * HD, SLAB_ROWS),
                probe_ref[rows, :],
                preferred_element_type=jnp.float32,
            ).reshape(STEP_HEADS, HD, PROBES)
            sums = jnp.sum(projected * lane_ref[...][None], axis=1)
            checks_ref[heads, slab, :] = sums
            total = total + sums
            if block + 1 < blocks and slab < per_block:
                flip(block + 1, slab)
        part_ref[block] = total.reshape(PART_ROWS, HD)
    for block in range(blocks):
        send_shards(block).wait()


def finish(arrived, place, lane, probe):
    vmem = pl.BlockSpec(memory_space=pltpu.VMEM)
    hbm = pl.BlockSpec(memory_space=pltpu.HBM)
    blocks = SLOTS // STEP_HEADS
    fetches = SLOTS // FETCH_HEADS
    return pl.pallas_call(
        finish_kernel,
        in_specs=[hbm, vmem, vmem, hbm],
        out_specs=[hbm, vmem, vmem],
        out_shape=[
            pltpu.HBM((SLOTS, HD, GROUP_ROWS), jnp.bfloat16),
            pltpu.VMEM((SLOTS, SLABS, PROBES), jnp.float32),
            pltpu.VMEM((blocks, PART_ROWS, HD), jnp.float32),
        ],
        scratch_shapes=[
            pltpu.VMEM((fetches, GROUP_ROWS, FETCH_HEADS * HD), jnp.bfloat16),
            pltpu.VMEM((GROUP_ROWS, PROBES), jnp.bfloat16),
            pltpu.VMEM((blocks, STEP_HEADS, HD, GROUP_ROWS), jnp.bfloat16),
            pltpu.VMEM((2, STEP_HEADS * HD, GROUP_ROWS), jnp.bfloat16),
            pltpu.SemaphoreType.DMA((fetches,)),
            pltpu.SemaphoreType.DMA(()),
            pltpu.SemaphoreType.DMA((blocks,)),
        ],
        compiler_params=pltpu.CompilerParams(vmem_limit_bytes=FINISH_VMEM),
        name="finish",
    )(in_hbm(arrived), in_vmem(place), in_vmem(lane), in_hbm(probe))


def ring_sum(part, axis):
    size = lax.axis_size(axis)
    others = [
        lax.ppermute(part, axis, [(i, (i + step) % size) for i in range(size)])
        for step in (3, 1, 2)
    ]
    return sum([part, *others])


def body(stored, row_map, probe, lane):
    my_group = lax.axis_index(DP)
    outgoing = pack(in_hbm(stored)).reshape(N_DP * N_MP, SUB_ROWS, SLOTS * HD)
    incoming = lax.all_to_all(outgoing, EXCHANGE, split_axis=0, concat_axis=0, tiled=True)
    arrived = incoming.reshape(GROUP_ROWS, SLOTS * HD)
    by_source = row_map.reshape(N_DP * N_MP, N_DP, SUB_ROWS)
    mine = lax.dynamic_index_in_dim(by_source, my_group, 1, keepdims=False)
    mine = mine.reshape(SIDE, SIDE, N_MP, SUB_ROWS).transpose(2, 1, 0, 3)
    local_row = mine.reshape(GROUP_ROWS, 1) - my_group * GROUP_ROWS
    place, lane_wide = stage(local_row, lane)
    shards, slab_checks, part = finish(arrived, place, lane_wide, probe)
    row = ring_sum(part, DP[1])
    total = ring_sum(row, DP[0])
    head_sums = total.reshape(SLOTS, PROBES) / (N_DP * SLABS)
    return shards, slab_checks, head_sums


def solution(mesh):
    finer = Mesh(mesh.devices.reshape(SIDE, SIDE, SIDE, 2), DP_MP)
    placed = (P(DP_MP, None), P(), P(DP, None), P())
    return jax.shard_map(
        body,
        mesh=finer,
        in_specs=placed,
        out_specs=(P(MP, None, DP), P(MP, DP, None), P(MP, None)),
        check_vma=False,
    )
```

```python
import jax
import jax.numpy as jnp
from jax import lax
from jax.experimental import pallas as pl
from jax.experimental.pallas import tpu as pltpu
from jax.sharding import Mesh
from jax.sharding import PartitionSpec as P

Q_HEADS = 128
KV_HEADS = 8
HD = 128
PROBES = 1024
SLABS = 8
N_DP = 16
N_MP = 8
PER_DEVICE = Q_HEADS // N_MP
SLOTS = PER_DEVICE + 2
SUB_ROWS = 8
ROWS_DEV = 128
GROUP_ROWS = 1024
SLAB_ROWS = GROUP_ROWS // SLABS
DP = ("dp_0", "dp_1")
MP = ("mp_0", "mp_1")
DP_MP = DP + MP
EXCHANGE = ("mp_0", "mp_1", "dp_1", "dp_0")
SIDE = 4
STEP_HEADS = 6
FETCH_HEADS = 3
PART_ROWS = STEP_HEADS * PROBES // HD
PACK_VMEM = 20 << 20
STAGE_VMEM = 8 << 20
FINISH_VMEM = 28 << 20


def in_vmem(array):
    return pltpu.with_memory_space_constraint(array, pltpu.VMEM)


def in_hbm(array):
    return pltpu.with_memory_space_constraint(array, pltpu.HBM)


def pack_kernel(stored_ref, out_ref, wide_ref, narrow_ref, in_sem, out_sem):
    query = PER_DEVICE * HD
    first_kv = Q_HEADS * HD

    def fetch(piece, start, width):
        columns = pl.ds(start, width)
        return pltpu.make_async_copy(
            stored_ref.at[:, columns], wide_ref.at[:, columns], in_sem.at[piece]
        )

    def send(m):
        return pltpu.make_async_copy(
            narrow_ref.at[m], out_ref.at[m], out_sem.at[m]
        )

    key_value = fetch(N_MP, first_kv, 2 * KV_HEADS * HD)
    queries = [fetch(m, m * query, query) for m in range(N_MP)]
    key_value.start()
    for copy in queries:
        copy.start()
    key_value.wait()
    def place(m, start, width, to):
        for y in range(SIDE):
            for x in range(SIDE):
                first = (y * SIDE + x) * SUB_ROWS
                part = wide_ref[first : first + SUB_ROWS, start : start + width]
                narrow_ref[m, x * SIDE + y, :, to : to + width] = part.astype(
                    jnp.bfloat16
                )

    for m in range(N_MP):
        key = first_kv + m * HD
        place(m, key, HD, query)
        place(m, key + KV_HEADS * HD, HD, query + HD)
        queries[m].wait()
        place(m, m * query, query, 0)
        send(m).start()
    for m in range(N_MP):
        send(m).wait()


def pack(stored):
    return pl.pallas_call(
        pack_kernel,
        in_specs=[pl.BlockSpec(memory_space=pltpu.HBM)],
        out_specs=pl.BlockSpec(memory_space=pltpu.HBM),
        out_shape=pltpu.HBM((N_MP, N_DP, SUB_ROWS, SLOTS * HD), jnp.bfloat16),
        scratch_shapes=[
            pltpu.VMEM((ROWS_DEV, (Q_HEADS + 2 * KV_HEADS) * HD), jnp.float32),
            pltpu.VMEM((N_MP, N_DP, SUB_ROWS, SLOTS * HD), jnp.bfloat16),
            pltpu.SemaphoreType.DMA((N_MP + 1,)),
            pltpu.SemaphoreType.DMA((N_MP,)),
        ],
        compiler_params=pltpu.CompilerParams(vmem_limit_bytes=PACK_VMEM),
        name="pack",
    )(stored)


def stage_kernel(row_ref, lane_ref, place_ref, lane_out):
    targets = lax.broadcasted_iota(jnp.int32, (GROUP_ROWS, GROUP_ROWS), 1)
    place_ref[...] = jnp.where(row_ref[...] == targets, 1.0, 0.0).astype(jnp.bfloat16)
    lane_out[...] = lane_ref[...].astype(jnp.float32)


def stage(local_row, lane):
    vmem = pl.BlockSpec(memory_space=pltpu.VMEM)
    return pl.pallas_call(
        stage_kernel,
        in_specs=[vmem] * 2,
        out_specs=[vmem] * 2,
        out_shape=[
            pltpu.VMEM((GROUP_ROWS, GROUP_ROWS), jnp.bfloat16),
            pltpu.VMEM((HD, PROBES), jnp.float32),
        ],
        compiler_params=pltpu.CompilerParams(vmem_limit_bytes=STAGE_VMEM),
        cost_estimate=pl.CostEstimate(
            flops=1 << 30, bytes_accessed=8 << 20, transcendentals=0
        ),
        name="stage",
    )(local_row, in_hbm(lane))


def finish_kernel(
    arrived_hbm, place_ref, lane_ref, probe_hbm, shards_hbm, checks_ref, part_ref,
    arrived_ref, probe_ref, shards_ref, flipped_ref, in_sem, probe_sem, out_sem,
):
    width = FETCH_HEADS * HD
    fetches = SLOTS // FETCH_HEADS
    blocks = SLOTS // STEP_HEADS
    per_block = STEP_HEADS // FETCH_HEADS

    def fetch(piece):
        return pltpu.make_async_copy(
            arrived_hbm.at[:, pl.ds(piece * width, width)],
            arrived_ref.at[piece],
            in_sem.at[piece],
        )

    def send_shards(block):
        heads = pl.ds(block * STEP_HEADS, STEP_HEADS)
        return pltpu.make_async_copy(
            shards_ref.at[block], shards_hbm.at[heads], out_sem.at[block]
        )

    def flip(block, piece):
        rows = slice(piece * width, (piece + 1) * width)
        flipped_ref[block % 2, rows] = arrived_ref[block * per_block + piece].T

    probe_copy = pltpu.make_async_copy(probe_hbm, probe_ref, probe_sem)
    for piece in range(per_block):
        fetch(piece).start()
    probe_copy.start()
    for piece in range(per_block):
        fetch(piece).wait()
        if piece == 0:
            for later in range(per_block, fetches):
                fetch(later).start()
        flip(0, piece)
    for block in range(blocks):
        placed = jnp.dot(
            flipped_ref[block % 2], place_ref[...], preferred_element_type=jnp.float32
        ).astype(jnp.bfloat16)
        shards_ref[block] = placed.reshape(STEP_HEADS, HD, GROUP_ROWS)
        send_shards(block).start()
        if block == 0:
            probe_copy.wait()
            for piece in range(per_block, fetches):
                fetch(piece).wait()
        total = jnp.zeros((STEP_HEADS, PROBES), jnp.float32)
        heads = slice(block * STEP_HEADS, (block + 1) * STEP_HEADS)
        for slab in range(SLABS):
            rows = slice(slab * SLAB_ROWS, (slab + 1) * SLAB_ROWS)
            projected = jnp.dot(
                shards_ref[block, :, :, rows].reshape(STEP_HEADS * HD, SLAB_ROWS),
                probe_ref[rows, :],
                preferred_element_type=jnp.float32,
            ).reshape(STEP_HEADS, HD, PROBES)
            sums = jnp.sum(projected * lane_ref[...][None], axis=1)
            checks_ref[heads, slab, :] = sums
            total = total + sums
            if block + 1 < blocks and slab < per_block:
                flip(block + 1, slab)
        part_ref[block] = total.reshape(PART_ROWS, HD)
    for block in range(blocks):
        send_shards(block).wait()


def finish(arrived, place, lane, probe):
    vmem = pl.BlockSpec(memory_space=pltpu.VMEM)
    hbm = pl.BlockSpec(memory_space=pltpu.HBM)
    blocks = SLOTS // STEP_HEADS
    fetches = SLOTS // FETCH_HEADS
    return pl.pallas_call(
        finish_kernel,
        in_specs=[hbm, vmem, vmem, hbm],
        out_specs=[hbm, vmem, vmem],
        out_shape=[
            pltpu.HBM((SLOTS, HD, GROUP_ROWS), jnp.bfloat16),
            pltpu.VMEM((SLOTS, SLABS, PROBES), jnp.float32),
            pltpu.VMEM((blocks, PART_ROWS, HD), jnp.float32),
        ],
        scratch_shapes=[
            pltpu.VMEM((fetches, GROUP_ROWS, FETCH_HEADS * HD), jnp.bfloat16),
            pltpu.VMEM((GROUP_ROWS, PROBES), jnp.bfloat16),
            pltpu.VMEM((blocks, STEP_HEADS, HD, GROUP_ROWS), jnp.bfloat16),
            pltpu.VMEM((2, STEP_HEADS * HD, GROUP_ROWS), jnp.bfloat16),
            pltpu.SemaphoreType.DMA((fetches,)),
            pltpu.SemaphoreType.DMA(()),
            pltpu.SemaphoreType.DMA((blocks,)),
        ],
        compiler_params=pltpu.CompilerParams(vmem_limit_bytes=FINISH_VMEM),
        name="finish",
    )(in_hbm(arrived), in_vmem(place), in_vmem(lane), in_hbm(probe))


def ring_sum(part, axis):
    size = lax.axis_size(axis)
    others = [
        lax.ppermute(part, axis, [(i, (i + step) % size) for i in range(size)])
        for step in (3, 1, 2)
    ]
    return sum([part, *others])


def body(stored, row_map, probe, lane):
    my_group = lax.axis_index(DP)
    outgoing = pack(in_hbm(stored)).reshape(N_DP * N_MP, SUB_ROWS, SLOTS * HD)
    incoming = lax.all_to_all(outgoing, EXCHANGE, split_axis=0, concat_axis=0, tiled=True)
    arrived = incoming.reshape(GROUP_ROWS, SLOTS * HD)
    by_source = row_map.reshape(N_DP * N_MP, N_DP, SUB_ROWS)
    mine = lax.dynamic_index_in_dim(by_source, my_group, 1, keepdims=False)
    mine = mine.reshape(SIDE, SIDE, N_MP, SUB_ROWS).transpose(2, 1, 0, 3)
    local_row = mine.reshape(GROUP_ROWS, 1) - my_group * GROUP_ROWS
    place, lane_wide = stage(local_row, lane)
    shards, slab_checks, part = finish(arrived, place, lane_wide, probe)
    row = ring_sum(part, DP[1])
    total = ring_sum(row, DP[0])
    head_sums = total.reshape(SLOTS, PROBES) / (N_DP * SLABS)
    return shards, slab_checks, head_sums


def solution(mesh):
    finer = Mesh(mesh.devices.reshape(SIDE, SIDE, SIDE, 2), DP_MP)
    placed = (P(DP_MP, None), P(), P(DP, None), P())
    return jax.shard_map(
        body,
        mesh=finer,
        in_specs=placed,
        out_specs=(P(MP, None, DP), P(MP, DP, None), P(MP, None)),
        check_vma=False,
    )
```
